32 devices in a mesh: gz: 16 (over z, y, core), gy: 2 (over x).
Axes of the slice: x: 2, y: 2, z: 4, core: 2. Of those that a mesh axis runs over, the one named last changes fastest.
Arguments:
- fixed_image: float32 [160, 80, 320], P('gz', 'gy'), may hold values from -6 to 6
- moving_image: float32 [160, 80, 320], P('gz', 'gy'), may hold values from -6 to 6
- moving_grad: float32 [3, 160, 80, 320], P(None, 'gz', 'gy'), may hold values from -6 to 6
Outputs:
- control_grad: float32 [32, 3, 16, 64], P('gz', None, 'gy')
The draws below stay inside these ranges and needn't reach their ends.
All inputs are finite; a program needn't handle non-finite values.
Results may differ from the reference program's by a relative error of at most 0.00016.
Values sent between devices are 32-bit elements; how exact they have to be, the bound alone decides.
A program may use at most 64 MiB of HBM per device.

```python
import jax
import jax.numpy as jnp
from jax import lax

NX = 320
RADIUS = 4
SPACING = 5
NZ = 160
NY = 80
CZ = 32
CY = 16
CX = 64


def block_levels(key, shape, split, smallest, top_value):
    level, own = 1.0, jax.random.fold_in(key, 6)
    for axis_at, shards_of in split:
        heights = jnp.exp(jax.random.uniform(jax.random.fold_in(own, axis_at), (shards_of,), jnp.float32, smallest / len(split), top_value / len(split)))
        level = level * jnp.repeat(heights, shape[axis_at] // shards_of).reshape([-1 if axis == axis_at else 1 for axis in range(len(shape))])
    return level


def bell_draw(rng, extent, scale, limit, cuts=(), held_as=jnp.bfloat16):
    factor_of = block_levels(rng, extent, cuts, -0.22, 0.18) if cuts else 1.0
    entries = jax.random.normal(rng, extent, jnp.float32) * scale * factor_of
    return jnp.minimum(jnp.maximum(entries, -limit), limit).astype(held_as)


def setup_inputs(seed: int = 0) -> dict:
    arg_keys = jax.random.split(jax.random.key(seed), 4)
    return {
        "fixed_image": bell_draw(arg_keys[0], (NZ, NY, NX), 1.0, 6.0, ((0, 16), (1, 2)), jnp.float32),
        "moving_image": bell_draw(arg_keys[1], (NZ, NY, NX), 1.0, 6.0, ((0, 16), (1, 2)), jnp.float32),
        "moving_grad": bell_draw(arg_keys[2], (3, NZ, NY, NX), 1.0, 6.0, ((1, 16), (2, 2)), jnp.float32),
    }


EPS = 36.0
SIM_WEIGHT = 8.0


def spline_basis(voxels, points, anchor, first_point, columns):
    position = anchor + jnp.arange(voxels, dtype=jnp.int32)
    cell_index = position // SPACING
    fraction = (position - cell_index * SPACING).astype(jnp.float32) / SPACING
    remainder = 1.0 - fraction
    weights = [remainder ** 3 / 6.0,
               (3.0 * fraction ** 3 - 6.0 * fraction ** 2 + 4.0) / 6.0,
               (-3.0 * fraction ** 3 + 3.0 * fraction ** 2 + 3.0 * fraction + 1.0) / 6.0,
               fraction ** 3 / 6.0]
    targets = first_point + jnp.arange(columns, dtype=jnp.int32)
    matrix = jnp.zeros((voxels, columns), jnp.float32)
    for spline in range(4):
        clamped = jnp.clip(cell_index - 1 + spline, 0, points - 1)
        matrix = matrix + weights[spline][:, None] * (clamped[:, None] == targets[None, :]).astype(jnp.float32)
    return matrix


def box_axis(values, dimension):
    length = values.shape[dimension]
    widths = [(0, 0)] * values.ndim
    widths[dimension] = (RADIUS, RADIUS)
    padded = jnp.pad(values, widths)
    running = lax.slice_in_dim(padded, 0, length, axis=dimension)
    for offset in range(1, 2 * RADIUS + 1):
        running = running + lax.slice_in_dim(padded, offset, offset + length, axis=dimension)
    return running


def box_full(values):
    return box_axis(box_axis(box_axis(values, 2), 1), 0)


def reference(fixed_image, moving_image, moving_grad):
    fixed_part = fixed_image.astype(jnp.float32)
    moving_part = moving_image.astype(jnp.float32)
    window_size = float((2 * RADIUS + 1) ** 3)
    sum_f = box_full(fixed_part)
    sum_m = box_full(moving_part)
    sum_ff = box_full(fixed_part * fixed_part)
    sum_mm = box_full(moving_part * moving_part)
    sum_fm = box_full(fixed_part * moving_part)
    covariance = sum_fm - sum_f * sum_m / window_size
    variance_fixed = sum_ff - sum_f * sum_f / window_size + EPS
    variance_moving = sum_mm - sum_m * sum_m / window_size + EPS
    quotient = covariance / (variance_fixed * variance_moving)
    weight_cross = 2.0 * quotient
    weight_moving = -quotient * covariance / variance_moving
    boxed_one = box_full(weight_cross)
    boxed_two = box_full(weight_cross * sum_f / window_size)
    boxed_three = box_full(weight_moving)
    boxed_four = box_full(weight_moving * sum_m / window_size)
    similarity_slope = -SIM_WEIGHT * (fixed_part * boxed_one - boxed_two + 2.0 * moving_part * boxed_three - 2.0 * boxed_four)
    basis_x = spline_basis(NX, CX, 0, 0, CX)
    basis_y = spline_basis(NY, CY, 0, 0, CY)
    basis_z = spline_basis(NZ, CZ, 0, 0, CZ)
    results = []
    for component in range(3):
        voxel_grad = similarity_slope * moving_grad[component].astype(jnp.float32)
        along_x = jnp.dot(voxel_grad.reshape(-1, NX), basis_x, precision=lax.Precision.HIGHEST).reshape(NZ, NY, CX)
        along_y = jnp.einsum("zyx,yb->zbx", along_x, basis_y, precision=lax.Precision.HIGHEST)
        results.append(jnp.einsum("zbx,zq->qbx", along_y, basis_z, precision=lax.Precision.HIGHEST))
    return jnp.stack(results, axis=1)
```

```python
import functools

import jax
import jax.numpy as jnp
import numpy as np
from jax import lax
from jax.experimental import pallas as pl
from jax.experimental.pallas import tpu as pltpu
from jax.sharding import PartitionSpec as P

RADIUS = 4
SPACING = 5
EPS = 36.0
SIM_WEIGHT = 8.0
WINDOW = float((2 * RADIUS + 1) ** 3)
HALO = 2 * RADIUS
MESH = pl.DeviceIdType.MESH


def spline_matrix(voxels, points):
    position = np.arange(voxels)
    cell = position // SPACING
    u = (position - cell * SPACING) / SPACING
    weights = [
        (1 - u) ** 3 / 6,
        (3 * u**3 - 6 * u**2 + 4) / 6,
        (-3 * u**3 + 3 * u**2 + 3 * u + 1) / 6,
        u**3 / 6,
    ]
    matrix = np.zeros((voxels, points))
    for k in range(4):
        np.add.at(matrix, (position, np.clip(cell - 1 + k, 0, points - 1)), weights[k])
    return matrix


def window_sum(v, axis, leading):
    n = v.shape[axis]

    def moved(a, s):
        return pltpu.roll(a, n - s if leading else s, axis)

    two = v + moved(v, 1)
    four = two + moved(two, 2)
    eight = four + moved(four, 4)
    return eight + moved(v, 8)


def split(v):
    hi = v.astype(jnp.bfloat16)
    return hi, (v - hi.astype(jnp.float32)).astype(jnp.bfloat16)


def dot(a, b):
    return jnp.dot(a, b, preferred_element_type=jnp.float32)


def kernel(
    gz_count, planes, height, width, points_y, points_x,
    bz_ref, fixed_ref, moving_ref, grad_ref, bx_ref, by_ref, out_ref,
    ext, grad, sums, boxes, coef, ksum, slope, acc, part, arrived,
    local_sem, z_send, z_recv, y_send, y_recv, p_send, p_recv,
):
    z, g = lax.axis_index("gz"), lax.axis_index("gy")
    other = 1 - g
    up, down = z < gz_count - 1, z > 0
    rows, lanes = slope.shape
    y0 = pl.multiple_of(g * HALO, 8)
    y_src = pl.multiple_of(jnp.where(g == 0, height - HALO, HALO), 8)
    y_dst = pl.multiple_of(jnp.where(g == 0, 0, height), 8)
    own_src = pl.multiple_of(jnp.where(g == 0, height - HALO, 0), 8)
    owned = planes // SPACING
    cols = owned + 3
    images = (fixed_ref, moving_ref)

    def window(p, i):
        return ext.at[i, p, pl.ds(y0, height)]

    local = [
        pltpu.make_async_copy(
            images[i],
            ext.at[i, pl.ds(HALO, planes), pl.ds(y0, height)],
            local_sem.at[i],
        )
        for i in range(2)
    ] + [pltpu.make_async_copy(grad_ref, grad, local_sem.at[2])]

    ext[:, :, rows - 8 :, :] = jnp.zeros((2, ext.shape[1], 8, width), jnp.float32)

    @pl.when(jnp.logical_not(down))
    def _():
        ext[:, 0:HALO] = jnp.zeros((2, HALO, rows, width), jnp.float32)

    @pl.when(jnp.logical_not(up))
    def _():
        ext[:, HALO + planes :] = jnp.zeros((2, HALO, rows, width), jnp.float32)

    barrier = pltpu.get_barrier_semaphore()

    def greet(cond, dz, gy):
        @pl.when(cond)
        def _():
            pl.semaphore_signal(barrier, 1, device_id={"gz": z + dz, "gy": gy}, device_id_type=MESH)

    pl.semaphore_signal(barrier, 1, device_id={"gz": z, "gy": other}, device_id_type=MESH)
    for gy in (g, other):
        greet(up, 1, gy)
        greet(down, -1, gy)
    pl.semaphore_wait(barrier, 1 + 2 * up.astype(jnp.int32) + 2 * down.astype(jnp.int32))

    def z_copy(i, d, s):
        src = planes - 1 - s if d == 0 else s
        dst = HALO - 1 - s if d == 0 else HALO + planes + s
        return pltpu.make_async_remote_copy(
            images[i].at[src], window(dst, i),
            z_send.at[i, d, s], z_recv.at[i, d, s],
            device_id={"gz": z + 1 if d == 0 else z - 1, "gy": g}, device_id_type=MESH,
        )

    def y_own(i):
        return pltpu.make_async_remote_copy(
            images[i].at[:, pl.ds(own_src, HALO), :],
            ext.at[i, pl.ds(HALO, planes), pl.ds(y_dst, HALO)],
            y_send.at[2, i], y_recv.at[2, i],
            device_id={"gz": z, "gy": other}, device_id_type=MESH,
        )

    def y_relay(d, s):
        p = HALO - 1 - s if d == 0 else HALO + planes + s
        return pltpu.make_async_remote_copy(
            ext.at[:, p, pl.ds(y_src, HALO)],
            ext.at[:, p, pl.ds(y_dst, HALO)],
            y_send.at[d, s], y_recv.at[d, s],
            device_id={"gz": z, "gy": other}, device_id_type=MESH,
        )

    sends = (up, down)
    takes = (down, up)

    for i in range(2):
        local[i].start()
        y_own(i).start()
    for d in range(2):
        @pl.when(sends[d])
        def _():
            for s in range(HALO):
                for i in range(2):
                    z_copy(i, d, s).start()
    local[2].start()
    for i in range(2):
        local[i].wait()
        y_own(i).wait_recv()

    def relay(s):
        for d in range(2):
            @pl.when(takes[d])
            def _():
                for i in range(2):
                    z_copy(i, d, s).wait_recv()
                y_relay(d, s).start()

    def ready(d, s):
        @pl.when(takes[d])
        def _():
            y_relay(d, s).wait_recv()

    pad = jnp.zeros((rows, lanes - width), jnp.float32)

    def plane(i, p):
        return jnp.concatenate([ext[i, p], pad], axis=1)

    def fields(p):
        f, m = plane(0, p), plane(1, p)
        return f, m, f * f, m * m, f * m

    row = lax.broadcasted_iota(jnp.int32, (rows, lanes), 0)
    lane = lax.broadcasted_iota(jnp.int32, (rows, lanes), 1)
    inside = (row >= RADIUS) & (row < rows - RADIUS) & (lane >= RADIUS) & (lane < width + RADIUS)

    def coefficients(way, k):
        for i in range(5):
            boxes[i] = window_sum(window_sum(sums[way, i], 0, False), 1, False)
        sf, sm = boxes[0], boxes[1]
        cov = boxes[4] - sf * sm * (1.0 / WINDOW)
        var_f = boxes[2] - sf * sf * (1.0 / WINDOW) + EPS
        var_m = boxes[3] - sm * sm * (1.0 / WINDOW) + EPS
        at = z * planes + k - RADIUS
        valid = (at >= 0) & (at < gz_count * planes)
        keep = jnp.where(valid, 1.0, 0.0)
        inv = 1.0 / (var_f * var_m)
        q = jnp.where(inside, cov * inv * keep, 0.0)
        h = q * cov * (var_f * inv)
        coef[0, k] = q
        coef[1, k] = h
        coef[2, k] = (q * sf - h * sm) * (1.0 / WINDOW)

    for i in range(5):
        sums[0, i] = jnp.zeros((rows, lanes), jnp.float32)

    @pl.loop(0, HALO + 1)
    def _(p):
        for i, v in enumerate(fields(HALO + p)):
            sums[0, i] += v

    sums[1] = sums[0]
    coefficients(0, HALO)

    def move(way, new, old, k):
        for i, (a, b) in enumerate(zip(fields(new), fields(old))):
            sums[way, i] += a - b
        coefficients(way, k)

    first = planes - 1 - HALO
    for j in range(first):
        move(0, 2 * HALO + 1 + j, HALO + j, HALO + 1 + j)

    relay(0)

    @pl.loop(0, HALO)
    def _(s):
        @pl.when(s < HALO - 1)
        def _():
            relay(s + 1)

        ready(0, s)
        move(1, HALO - 1 - s, 2 * HALO - s, HALO - 1 - s)
        ready(1, s)
        move(0, HALO + planes + s, planes - 1 + s, planes + s)

    for i in range(3):
        ksum[i] = jnp.zeros((rows, lanes), jnp.float32)
    acc[...] = jnp.zeros(acc.shape, jnp.float32)

    @pl.loop(0, HALO)
    def _(k):
        for i in range(3):
            ksum[i] += coef[i, k]

    local[2].wait()
    for cell in range(owned):
        @pl.loop(cell * SPACING, (cell + 1) * SPACING)
        def _(o):
            boxed = []
            for i in range(3):
                total = ksum[i] + coef[i, o + HALO]
                ksum[i] = total - coef[i, o]
                boxed.append(window_sum(window_sum(total, 0, True), 1, True))
            slope[...] = (-2.0 * SIM_WEIGHT) * (
                plane(0, o + HALO) * boxed[0] - plane(1, o + HALO) * boxed[1] - boxed[2]
            )
            own = slope[pl.ds(y0, height), 0:width]
            for c in range(3):
                v = own * grad[c, o]
                for j in range(cell, cell + 4):
                    acc[c * cols + j] += bz_ref[z * planes + o, j] * v

    for c in range(3):
        v = acc[c * cols : (c + 1) * cols].reshape(cols * height, width)
        hi, lo = split(v)
        along_x = dot(hi, bx_ref[0]) + dot(hi, bx_ref[1]) + dot(lo, bx_ref[0])
        hi, lo = split(along_x)
        by_hi, by_lo = by_ref[g, 0], by_ref[g, 1]
        along_y = dot(by_hi, hi) + dot(by_lo, hi) + dot(by_hi, lo)
        half = points_y // 2
        for j in range(cols):
            for h in range(2):
                at = j * points_y + h * half
                part[h, j, c] = along_y[at : at + half]

    def p_copy(slot, half, first_row, count, dz, gy):
        return pltpu.make_async_remote_copy(
            part.at[half, pl.ds(first_row, count)],
            arrived.at[slot, pl.ds(0, count)],
            p_send.at[slot], p_recv.at[slot],
            device_id={"gz": z + dz, "gy": gy}, device_id_type=MESH,
        )

    partner = p_copy(0, other, 1, owned, 0, other)
    ups = [p_copy(1, g, 1 + owned, 2, 1, g), p_copy(2, other, 1 + owned, 2, 1, other)]
    downs = [p_copy(3, g, 0, 1, -1, g), p_copy(4, other, 0, 1, -1, other)]

    @pl.when(up)
    def _():
        for copy in ups:
            copy.start()

    @pl.when(down)
    def _():
        for copy in downs:
            copy.start()

    partner.start()
    partner.wait_recv()
    out_ref[...] = part[g, 1 : 1 + owned] + arrived[0]

    @pl.when(down)
    def _():
        for copy in ups:
            copy.wait_recv()
        out_ref[0:2] += arrived[1, 0:2] + arrived[2, 0:2]

    @pl.when(up)
    def _():
        for copy in downs:
            copy.wait_recv()
        out_ref[owned - 1 : owned] += arrived[3, 0:1] + arrived[4, 0:1]

    partner.wait_send()
    for i in range(2):
        y_own(i).wait_send()

    @pl.when(up)
    def _():
        for copy in ups:
            copy.wait_send()

    @pl.when(down)
    def _():
        for copy in downs:
            copy.wait_send()

    for d in range(2):
        @pl.when(sends[d])
        def _():
            for s in range(HALO):
                for i in range(2):
                    z_copy(i, d, s).wait_send()

        @pl.when(takes[d])
        def _():
            for s in range(HALO):
                y_relay(d, s).wait_send()


def hi_lo(matrix):
    hi = matrix.astype(jnp.bfloat16)
    lo = (matrix - hi.astype(np.float64)).astype(jnp.bfloat16)
    return np.stack([hi, lo])


def local(gz_count, gy_count, fixed_image, moving_image, moving_grad):
    planes, height, width = fixed_image.shape
    points_x, points_y = width // SPACING, gy_count * height // SPACING
    depth = gz_count * planes
    owned = planes // SPACING
    cols = owned + 3
    assert gy_count == 2 and planes >= HALO + 1 and owned >= 2 and height % 8 == 0
    bx = hi_lo(spline_matrix(width, points_x))
    by_all = spline_matrix(gy_count * height, points_y)
    by = np.stack(
        [hi_lo(np.kron(np.eye(cols), by_all[h * height : (h + 1) * height].T)) for h in range(2)]
    )
    bz_all = np.pad(spline_matrix(depth, depth // SPACING), ((0, 0), (1, 2)))
    bz = np.stack(
        [bz_all[p, (p // planes) * owned : (p // planes) * owned + cols] for p in range(depth)]
    ).astype(np.float32)
    rows = height + 2 * HALO
    lanes = (width + HALO + 127) // 128 * 128
    ext_planes = planes + 2 * HALO
    f32 = jnp.float32
    body = functools.partial(kernel, gz_count, planes, height, width, points_y, points_x)
    vmem, smem, anyw = (pl.BlockSpec(memory_space=m) for m in (pltpu.VMEM, pltpu.SMEM, pl.ANY))
    half = points_y // 2
    return pl.pallas_call(
        body,
        out_shape=jax.ShapeDtypeStruct((owned, 3, half, points_x), f32),
        in_specs=[smem, anyw, anyw, anyw, vmem, vmem],
        out_specs=vmem,
        scratch_shapes=[
            pltpu.VMEM((2, ext_planes, rows, width), f32),
            pltpu.VMEM(moving_grad.shape, f32),
            pltpu.VMEM((2, 5, rows, lanes), f32),
            pltpu.VMEM((5, rows, lanes), f32),
            pltpu.VMEM((3, planes + HALO, rows, lanes), f32),
            pltpu.VMEM((3, rows, lanes), f32),
            pltpu.VMEM((rows, lanes), f32),
            pltpu.VMEM((3 * cols, height, width), f32),
            pltpu.VMEM((2, cols, 3, half, points_x), f32),
            pltpu.VMEM((5, owned, 3, half, points_x), f32),
            pltpu.SemaphoreType.DMA((3,)),
            pltpu.SemaphoreType.DMA((2, 2, HALO)),
            pltpu.SemaphoreType.DMA((2, 2, HALO)),
            pltpu.SemaphoreType.DMA((3, HALO)),
            pltpu.SemaphoreType.DMA((3, HALO)),
            pltpu.SemaphoreType.DMA((5,)),
            pltpu.SemaphoreType.DMA((5,)),
        ],
        compiler_params=pltpu.CompilerParams(
            collective_id=0, has_side_effects=True, vmem_limit_bytes=40 * 2**20
        ),
    )(jnp.asarray(bz), fixed_image, moving_image, moving_grad, jnp.asarray(bx), jnp.asarray(by))


def solution(mesh):
    in_specs = (P("gz", "gy", None), P("gz", "gy", None), P(None, "gz", "gy", None))
    out_specs = P("gz", None, "gy", None)
    body = functools.partial(local, mesh.shape["gz"], mesh.shape["gy"])
    return jax.shard_map(body, mesh=mesh, in_specs=in_specs, out_specs=out_specs, check_vma=False)
```

```python
import functools

import jax
import jax.numpy as jnp
import numpy as np
from jax import lax
from jax.experimental import pallas as pl
from jax.experimental.pallas import tpu as pltpu
from jax.sharding import PartitionSpec as P

RADIUS = 4
SPACING = 5
EPS = 36.0
SIM_WEIGHT = 8.0
WINDOW = float((2 * RADIUS + 1) ** 3)
HALO = 2 * RADIUS
MESH = pl.DeviceIdType.MESH


def spline_weights(u):
    v = 1.0 - u
    return [
        v * v * v * (1.0 / 6.0),
        (3.0 * u * u * u - 6.0 * u * u + 4.0) * (1.0 / 6.0),
        (-3.0 * u * u * u + 3.0 * u * u + 3.0 * u + 1.0) * (1.0 / 6.0),
        u * u * u * (1.0 / 6.0),
    ]


def spline_matrix(voxels, points):
    position = np.arange(voxels)
    cell = position // SPACING
    u = (position - cell * SPACING) / SPACING
    weights = spline_weights(u)
    matrix = np.zeros((voxels, points))
    for k in range(4):
        np.add.at(matrix, (position, np.clip(cell - 1 + k, 0, points - 1)), weights[k])
    return matrix


def window_sum(v, axis, leading):
    n = v.shape[axis]

    def moved(a, s):
        return pltpu.roll(a, n - s if leading else s, axis)

    two = v + moved(v, 1)
    four = two + moved(two, 2)
    eight = four + moved(four, 4)
    return eight + moved(v, 8)


def split(v):
    hi = v.astype(jnp.bfloat16)
    return hi, (v - hi.astype(jnp.float32)).astype(jnp.bfloat16)


def dot(a, b):
    return jnp.dot(a, b, preferred_element_type=jnp.float32)


def kernel(
    gz_count, planes, height, width, points_y, points_x,
    fixed_ref, moving_ref, grad_ref, bx_hbm, by_hbm, band_hbm, out_ref,
    bx_ref, by_ref, band, ext, grad, sums, boxes, coef, ksum, slope, acc, part, arrived,
    local_sem, z_send, z_recv, y_send, y_recv, p_send, p_recv,
):
    z, g = lax.axis_index("gz"), lax.axis_index("gy")
    other = 1 - g
    up, down = z < gz_count - 1, z > 0
    rows, lanes = slope.shape
    y0 = pl.multiple_of(g * HALO, 8)
    y_src = pl.multiple_of(jnp.where(g == 0, height - HALO, HALO), 8)
    y_dst = pl.multiple_of(jnp.where(g == 0, 0, height), 8)
    own_src = pl.multiple_of(jnp.where(g == 0, height - HALO, 0), 8)
    owned = planes // SPACING
    cols = owned + 3
    images = (fixed_ref, moving_ref)

    def window(p, i):
        return ext.at[i, p, pl.ds(y0, height)]

    local = [
        pltpu.make_async_copy(
            images[i],
            ext.at[i, pl.ds(HALO, planes), pl.ds(y0, height)],
            local_sem.at[i],
        )
        for i in range(2)
    ] + [pltpu.make_async_copy(grad_ref, grad, local_sem.at[2])]
    tables = [
        pltpu.make_async_copy(band_hbm, band, local_sem.at[3]),
        pltpu.make_async_copy(bx_hbm, bx_ref, local_sem.at[4]),
        pltpu.make_async_copy(by_hbm.at[g], by_ref, local_sem.at[5]),
    ]

    ext[:, :, rows - 8 :, :] = jnp.zeros((2, ext.shape[1], 8, width), jnp.float32)

    @pl.when(jnp.logical_not(down))
    def _():
        ext[:, 0:HALO] = jnp.zeros((2, HALO, rows, width), jnp.float32)

    @pl.when(jnp.logical_not(up))
    def _():
        ext[:, HALO + planes :] = jnp.zeros((2, HALO, rows, width), jnp.float32)

    barrier = pltpu.get_barrier_semaphore()

    def greet(cond, dz, gy):
        @pl.when(cond)
        def _():
            pl.semaphore_signal(barrier, 1, device_id={"gz": z + dz, "gy": gy}, device_id_type=MESH)

    pl.semaphore_signal(barrier, 1, device_id={"gz": z, "gy": other}, device_id_type=MESH)
    for gy in (g, other):
        greet(up, 1, gy)
        greet(down, -1, gy)
    pl.semaphore_wait(barrier, 1 + 2 * up.astype(jnp.int32) + 2 * down.astype(jnp.int32))

    def z_copy(i, d, s):
        src = planes - 1 - s if d == 0 else s
        dst = HALO - 1 - s if d == 0 else HALO + planes + s
        return pltpu.make_async_remote_copy(
            images[i].at[src], window(dst, i),
            z_send.at[i, d, s], z_recv.at[i, d, s],
            device_id={"gz": z + 1 if d == 0 else z - 1, "gy": g}, device_id_type=MESH,
        )

    def y_own(i):
        return pltpu.make_async_remote_copy(
            images[i].at[:, pl.ds(own_src, HALO), :],
            ext.at[i, pl.ds(HALO, planes), pl.ds(y_dst, HALO)],
            y_send.at[2, i], y_recv.at[2, i],
            device_id={"gz": z, "gy": other}, device_id_type=MESH,
        )

    def y_relay(d, s):
        p = HALO - 1 - s if d == 0 else HALO + planes + s
        return pltpu.make_async_remote_copy(
            ext.at[:, p, pl.ds(y_src, HALO)],
            ext.at[:, p, pl.ds(y_dst, HALO)],
            y_send.at[d, s], y_recv.at[d, s],
            device_id={"gz": z, "gy": other}, device_id_type=MESH,
        )

    sends = (up, down)
    takes = (down, up)

    for i in range(2):
        local[i].start()
        y_own(i).start()
    for d in range(2):
        @pl.when(sends[d])
        def _():
            for s in range(HALO):
                for i in range(2):
                    z_copy(i, d, s).start()
    for copy in (tables[0], local[2], tables[1], tables[2]):
        copy.start()
    for i in range(2):
        local[i].wait()
        y_own(i).wait_recv()
    tables[0].wait()

    def relay(s):
        for d in range(2):
            @pl.when(takes[d])
            def _():
                for i in range(2):
                    z_copy(i, d, s).wait_recv()
                y_relay(d, s).start()

    def ready(d, s):
        @pl.when(takes[d])
        def _():
            y_relay(d, s).wait_recv()

    pad = jnp.zeros((rows, lanes - width), jnp.float32)

    def plane(i, p):
        return jnp.concatenate([ext[i, p], pad], axis=1)

    def fields(p):
        f, m = plane(0, p), plane(1, p)
        return f, m, f * f, m * m, f * m

    row = lax.broadcasted_iota(jnp.int32, (rows, lanes), 0)
    lane = lax.broadcasted_iota(jnp.int32, (rows, lanes), 1)
    inside = (row >= RADIUS) & (row < rows - RADIUS) & (lane >= RADIUS) & (lane < width + RADIUS)

    def band_dots(v, at, mid, end):
        pieces = []
        for _ in range(3):
            piece = v.astype(jnp.bfloat16)
            v = v - piece.astype(jnp.float32)
            pieces.append(piece)
        left = sum(dot(p[:, 0:256], band[:, at:mid]) for p in pieces)
        right = sum(dot(p[:, 128:384], band[:, mid:end]) for p in pieces)
        return left, right

    def coefficients(way, k):
        left, right = band_dots(sums[way].reshape(5 * rows, lanes), 0, 256, 384)
        boxes[0 : 5 * rows, 0:256] = left
        boxes[0 : 5 * rows, 256:] = right
        sf, sm, sff, smm, sfm = (
            window_sum(boxes[i * rows : (i + 1) * rows], 0, False) for i in range(5)
        )
        cov = sfm - sf * sm * (1.0 / WINDOW)
        var_f = sff - sf * sf * (1.0 / WINDOW) + EPS
        var_m = smm - sm * sm * (1.0 / WINDOW) + EPS
        at = z * planes + k - RADIUS
        valid = (at >= 0) & (at < gz_count * planes)
        keep = jnp.where(valid, 1.0, 0.0)
        inv = 1.0 / (var_f * var_m)
        q = jnp.where(inside, cov * inv * keep, 0.0)
        h = q * cov * (var_f * inv)
        coef[0, k] = q
        coef[1, k] = h
        coef[2, k] = (q * sf - h * sm) * (1.0 / WINDOW)

    for i in range(5):
        sums[0, i] = jnp.zeros((rows, lanes), jnp.float32)

    @pl.loop(0, HALO + 1)
    def _(p):
        for i, v in enumerate(fields(HALO + p)):
            sums[0, i] += v

    sums[1] = sums[0]
    coefficients(0, HALO)

    def move(way, new, old, k):
        for i, (a, b) in enumerate(zip(fields(new), fields(old))):
            sums[way, i] += a - b
        coefficients(way, k)

    first = planes - 1 - HALO
    for j in range(first):
        move(0, 2 * HALO + 1 + j, HALO + j, HALO + 1 + j)

    relay(0)

    @pl.loop(0, HALO)
    def _(s):
        @pl.when(s < HALO - 1)
        def _():
            relay(s + 1)

        ready(0, s)
        move(1, HALO - 1 - s, 2 * HALO - s, HALO - 1 - s)
        ready(1, s)
        move(0, HALO + planes + s, planes - 1 + s, planes + s)

    for i in range(3):
        ksum[i] = jnp.zeros((rows, lanes), jnp.float32)
    acc[...] = jnp.zeros(acc.shape, jnp.float32)

    @pl.loop(0, HALO)
    def _(k):
        for i in range(3):
            ksum[i] += coef[i, k]

    local[2].wait()
    for cell in range(owned):
        @pl.loop(cell * SPACING, (cell + 1) * SPACING)
        def _(o):
            total = ksum[...] + coef[:, o + HALO]
            ksum[...] = total - coef[:, o]
            left, right = band_dots(total.reshape(3 * rows, lanes), 384, 512, 768)
            boxes[0 : 3 * rows, 0:128] = left
            boxes[0 : 3 * rows, 128:] = right
            boxed = [window_sum(boxes[i * rows : (i + 1) * rows], 0, True) for i in range(3)]
            slope[...] = (-2.0 * SIM_WEIGHT) * (
                plane(0, o + HALO) * boxed[0] - plane(1, o + HALO) * boxed[1] - boxed[2]
            )
            u = (o - cell * SPACING).astype(jnp.float32) * (1.0 / SPACING)
            weights = spline_weights(u)
            own = slope[pl.ds(y0, height), 0:width]
            for c in range(3):
                v = own * grad[c, o]
                for k in range(4):
                    acc[c * cols + cell + k] += weights[k] * v

    tables[1].wait()
    tables[2].wait()
    for c in range(3):
        v = acc[c * cols : (c + 1) * cols].reshape(cols * height, width)
        hi, lo = split(v)
        along_x = dot(hi, bx_ref[0]) + dot(hi, bx_ref[1]) + dot(lo, bx_ref[0])
        hi, lo = split(along_x)
        by_hi, by_lo = by_ref[0], by_ref[1]
        along_y = dot(by_hi, hi) + dot(by_lo, hi) + dot(by_hi, lo)
        half = points_y // 2
        for j in range(cols):
            for h in range(2):
                at = j * points_y + h * half
                part[h, j, c] = along_y[at : at + half]

    @pl.when(jnp.logical_not(down))
    def _():
        part[:, 1] += part[:, 0]

    @pl.when(jnp.logical_not(up))
    def _():
        part[:, owned] += part[:, owned + 1] + part[:, owned + 2]

    def p_copy(slot, half, first_row, count, dz, gy):
        return pltpu.make_async_remote_copy(
            part.at[half, pl.ds(first_row, count)],
            arrived.at[slot, pl.ds(0, count)],
            p_send.at[slot], p_recv.at[slot],
            device_id={"gz": z + dz, "gy": gy}, device_id_type=MESH,
        )

    partner = p_copy(0, other, 1, owned, 0, other)
    ups = [p_copy(1, g, 1 + owned, 2, 1, g), p_copy(2, other, 1 + owned, 2, 1, other)]
    downs = [p_copy(3, g, 0, 1, -1, g), p_copy(4, other, 0, 1, -1, other)]

    @pl.when(up)
    def _():
        for copy in ups:
            copy.start()

    @pl.when(down)
    def _():
        for copy in downs:
            copy.start()

    partner.start()
    partner.wait_recv()
    out_ref[...] = part[g, 1 : 1 + owned] + arrived[0]

    @pl.when(down)
    def _():
        for copy in ups:
            copy.wait_recv()
        out_ref[0:2] += arrived[1, 0:2] + arrived[2, 0:2]

    @pl.when(up)
    def _():
        for copy in downs:
            copy.wait_recv()
        out_ref[owned - 1 : owned] += arrived[3, 0:1] + arrived[4, 0:1]

    partner.wait_send()
    for i in range(2):
        y_own(i).wait_send()

    @pl.when(up)
    def _():
        for copy in ups:
            copy.wait_send()

    @pl.when(down)
    def _():
        for copy in downs:
            copy.wait_send()

    for d in range(2):
        @pl.when(sends[d])
        def _():
            for s in range(HALO):
                for i in range(2):
                    z_copy(i, d, s).wait_send()

        @pl.when(takes[d])
        def _():
            for s in range(HALO):
                y_relay(d, s).wait_send()


def hi_lo(matrix):
    hi = matrix.astype(jnp.bfloat16)
    lo = (matrix - hi.astype(np.float64)).astype(jnp.bfloat16)
    return np.stack([hi, lo])


def band_matrices():
    a, j = np.arange(256)[:, None], np.arange(384)[None, :]
    back = np.concatenate([(j - a)[:, :256], (j - a - 128)[:, 256:]], axis=1)
    ahead = np.concatenate([(a - j)[:, :128], (a + 128 - j)[:, 128:]], axis=1)
    shift = np.concatenate([back, ahead], axis=1)
    return ((shift >= 0) & (shift <= 2 * RADIUS)).astype(jnp.bfloat16)


def local(gz_count, gy_count, fixed_image, moving_image, moving_grad):
    planes, height, width = fixed_image.shape
    points_x, points_y = width // SPACING, gy_count * height // SPACING
    owned = planes // SPACING
    cols = owned + 3
    assert gy_count == 2 and planes >= HALO + 1 and owned >= 2 and height % 8 == 0
    bx = hi_lo(spline_matrix(width, points_x))
    by_all = spline_matrix(gy_count * height, points_y)
    by = np.stack(
        [hi_lo(np.kron(np.eye(cols), by_all[h * height : (h + 1) * height].T)) for h in range(2)]
    )
    rows = height + 2 * HALO
    lanes = (width + HALO + 127) // 128 * 128
    ext_planes = planes + 2 * HALO
    assert lanes == 384
    band = band_matrices()
    f32 = jnp.float32
    body = functools.partial(kernel, gz_count, planes, height, width, points_y, points_x)
    vmem, hbm = (pl.BlockSpec(memory_space=m) for m in (pltpu.VMEM, pltpu.HBM))
    half = points_y // 2
    return pl.pallas_call(
        body,
        out_shape=jax.ShapeDtypeStruct((owned, 3, half, points_x), f32),
        in_specs=[hbm] * 6,
        out_specs=vmem,
        scratch_shapes=[
            pltpu.VMEM(bx.shape, jnp.bfloat16),
            pltpu.VMEM(by.shape[1:], jnp.bfloat16),
            pltpu.VMEM(band.shape, jnp.bfloat16),
            pltpu.VMEM((2, ext_planes, rows, width), f32),
            pltpu.VMEM(moving_grad.shape, f32),
            pltpu.VMEM((2, 5, rows, lanes), f32),
            pltpu.VMEM((5 * rows, lanes), f32),
            pltpu.VMEM((3, planes + HALO, rows, lanes), f32),
            pltpu.VMEM((3, rows, lanes), f32),
            pltpu.VMEM((rows, lanes), f32),
            pltpu.VMEM((3 * cols, height, width), f32),
            pltpu.VMEM((2, cols, 3, half, points_x), f32),
            pltpu.VMEM((5, owned, 3, half, points_x), f32),
            pltpu.SemaphoreType.DMA((6,)),
            pltpu.SemaphoreType.DMA((2, 2, HALO)),
            pltpu.SemaphoreType.DMA((2, 2, HALO)),
            pltpu.SemaphoreType.DMA((3, HALO)),
            pltpu.SemaphoreType.DMA((3, HALO)),
            pltpu.SemaphoreType.DMA((5,)),
            pltpu.SemaphoreType.DMA((5,)),
        ],
        compiler_params=pltpu.CompilerParams(
            collective_id=0, has_side_effects=True, vmem_limit_bytes=40 * 2**20
        ),
    )(fixed_image, moving_image, moving_grad, jnp.asarray(bx), jnp.asarray(by), jnp.asarray(band))


def solution(mesh):
    in_specs = (P("gz", "gy", None), P("gz", "gy", None), P(None, "gz", "gy", None))
    out_specs = P("gz", None, "gy", None)
    body = functools.partial(local, mesh.shape["gz"], mesh.shape["gy"])
    return jax.shard_map(body, mesh=mesh, in_specs=in_specs, out_specs=out_specs, check_vma=False)
```

```python
import functools

import jax
import jax.numpy as jnp
import numpy as np
from jax import lax
from jax.experimental import pallas as pl
from jax.experimental.pallas import tpu as pltpu
from jax.sharding import PartitionSpec as P

RADIUS = 4
SPACING = 5
EPS = 36.0
SIM_WEIGHT = 8.0
WINDOW = float((2 * RADIUS + 1) ** 3)
HALO = 2 * RADIUS
MESH = pl.DeviceIdType.MESH


def spline_weights(u):
    v = 1.0 - u
    return [
        v * v * v * (1.0 / 6.0),
        (3.0 * u * u * u - 6.0 * u * u + 4.0) * (1.0 / 6.0),
        (-3.0 * u * u * u + 3.0 * u * u + 3.0 * u + 1.0) * (1.0 / 6.0),
        u * u * u * (1.0 / 6.0),
    ]


def spline_matrix(voxels, points):
    position = np.arange(voxels)
    cell = position // SPACING
    u = (position - cell * SPACING) / SPACING
    weights = spline_weights(u)
    matrix = np.zeros((voxels, points))
    for k in range(4):
        np.add.at(matrix, (position, np.clip(cell - 1 + k, 0, points - 1)), weights[k])
    return matrix


def window_sum(v, axis, leading):
    n = v.shape[axis]

    def moved(a, s):
        return pltpu.roll(a, n - s if leading else s, axis)

    two = v + moved(v, 1)
    four = two + moved(two, 2)
    eight = four + moved(four, 4)
    return eight + moved(v, 8)


def split(v):
    hi = v.astype(jnp.bfloat16)
    return hi, (v - hi.astype(jnp.float32)).astype(jnp.bfloat16)


def dot(a, b):
    return jnp.dot(a, b, preferred_element_type=jnp.float32)


def kernel(
    gz_count, planes, height, width, points_y, points_x,
    fixed_ref, moving_ref, grad_ref, bx_hbm, by_hbm, band_hbm, out_ref,
    bx_ref, by_ref, band, raw, ext, grad, sums, boxes, coef, ksum, slope, acc, part, arrived,
    local_sem, z_send, z_recv, y_send, y_recv, p_send, p_recv,
):
    z, g = lax.axis_index("gz"), lax.axis_index("gy")
    other = 1 - g
    up, down = z < gz_count - 1, z > 0
    rows, lanes = slope.shape
    y0 = pl.multiple_of(g * HALO, 8)
    y_src = pl.multiple_of(jnp.where(g == 0, height - HALO, HALO), 8)
    y_dst = pl.multiple_of(jnp.where(g == 0, 0, height), 8)
    owned = planes // SPACING
    cols = owned + 3
    images = (fixed_ref, moving_ref)

    local = [pltpu.make_async_copy(images[i], raw.at[i], local_sem.at[i]) for i in range(2)]
    local.append(pltpu.make_async_copy(grad_ref, grad, local_sem.at[2]))
    tables = [
        pltpu.make_async_copy(band_hbm, band, local_sem.at[3]),
        pltpu.make_async_copy(bx_hbm, bx_ref, local_sem.at[4]),
        pltpu.make_async_copy(by_hbm.at[g], by_ref, local_sem.at[5]),
    ]

    for copy in (*local, *tables):
        copy.start()

    ext_planes, packed = ext.shape[0], ext.shape[2]
    ext[:, rows - 8 :, :] = jnp.zeros((ext_planes, 8, packed), jnp.float32)

    @pl.when(jnp.logical_not(down))
    def _():
        ext[0:HALO] = jnp.zeros((HALO, rows, packed), jnp.float32)

    @pl.when(jnp.logical_not(up))
    def _():
        ext[HALO + planes :] = jnp.zeros((HALO, rows, packed), jnp.float32)

    barrier = pltpu.get_barrier_semaphore()

    def greet(cond, dz, gy):
        @pl.when(cond)
        def _():
            pl.semaphore_signal(barrier, 1, device_id={"gz": z + dz, "gy": gy}, device_id_type=MESH)

    pl.semaphore_signal(barrier, 1, device_id={"gz": z, "gy": other}, device_id_type=MESH)
    for gy in (g, other):
        greet(up, 1, gy)
        greet(down, -1, gy)
    for i in range(2):
        local[i].wait()
    tail = width - 256

    @pl.loop(0, planes)
    def _(p):
        at = (HALO + p, pl.ds(y0, height))
        ext[(*at, slice(0, 256))] = raw[0, p, :, 0:256]
        ext[(*at, slice(256, 512))] = raw[1, p, :, 0:256]
        ext[(*at, slice(512, 640))] = jnp.concatenate(
            [raw[0, p, :, 256:width], raw[1, p, :, 256:width]], axis=1
        )

    pl.semaphore_wait(barrier, 1 + 2 * up.astype(jnp.int32) + 2 * down.astype(jnp.int32))

    def z_copy(d, s):
        src = HALO + planes - 1 - s if d == 0 else HALO + s
        dst = HALO - 1 - s if d == 0 else HALO + planes + s
        return pltpu.make_async_remote_copy(
            ext.at[src, pl.ds(y0, height)], ext.at[dst, pl.ds(y0, height)],
            z_send.at[d, s], z_recv.at[d, s],
            device_id={"gz": z + 1 if d == 0 else z - 1, "gy": g}, device_id_type=MESH,
        )

    def y_copy(at, d, s):
        return pltpu.make_async_remote_copy(
            ext.at[at, pl.ds(y_src, HALO)], ext.at[at, pl.ds(y_dst, HALO)],
            y_send.at[d, s], y_recv.at[d, s],
            device_id={"gz": z, "gy": other}, device_id_type=MESH,
        )

    y_own = y_copy(pl.ds(HALO, planes), 2, 0)

    def y_relay(d, s):
        return y_copy(HALO - 1 - s if d == 0 else HALO + planes + s, d, s)

    sends = (up, down)
    takes = (down, up)

    y_own.start()
    for s in range(HALO):
        for d in range(2):
            @pl.when(sends[d])
            def _():
                z_copy(d, s).start()
    y_own.wait_recv()
    tables[0].wait()

    def relay(s):
        for d in range(2):
            @pl.when(takes[d])
            def _():
                z_copy(d, s).wait_recv()
                y_relay(d, s).start()

    def ready(d, s):
        @pl.when(takes[d])
        def _():
            y_relay(d, s).wait_recv()

    in_tail = lax.broadcasted_iota(jnp.int32, (rows, 128), 1) < tail

    def plane(i, p):
        last = ext[p, :, 512:640]
        if i == 1:
            last = pltpu.roll(last, 128 - tail, 1)
        last = jnp.where(in_tail, last, 0.0)
        return jnp.concatenate([ext[p, :, 256 * i : 256 * (i + 1)], last], axis=1)

    def fields(p):
        f, m = plane(0, p), plane(1, p)
        return f, m, f * f, m * m, f * m

    row = lax.broadcasted_iota(jnp.int32, (rows, lanes), 0)
    lane = lax.broadcasted_iota(jnp.int32, (rows, lanes), 1)
    inside = (row >= RADIUS) & (row < rows - RADIUS) & (lane >= RADIUS) & (lane < width + RADIUS)

    def band_dots(v, at, mid, end):
        pieces = []
        for _ in range(3):
            piece = v.astype(jnp.bfloat16)
            v = v - piece.astype(jnp.float32)
            pieces.append(piece)
        left = sum(dot(p[:, 0:256], band[:, at:mid]) for p in pieces)
        right = sum(dot(p[:, 128:384], band[:, mid:end]) for p in pieces)
        return left, right

    def coefficients(way, k):
        left, right = band_dots(sums[way].reshape(5 * rows, lanes), 0, 256, 384)
        boxes[0 : 5 * rows, 0:256] = left
        boxes[0 : 5 * rows, 256:] = right
        sf, sm, sff, smm, sfm = (
            window_sum(boxes[i * rows : (i + 1) * rows], 0, False) for i in range(5)
        )
        cov = sfm - sf * sm * (1.0 / WINDOW)
        var_f = sff - sf * sf * (1.0 / WINDOW) + EPS
        var_m = smm - sm * sm * (1.0 / WINDOW) + EPS
        at = z * planes + k - RADIUS
        valid = (at >= 0) & (at < gz_count * planes)
        keep = jnp.where(valid, 1.0, 0.0)
        inv = 1.0 / (var_f * var_m)
        q = jnp.where(inside, cov * inv * keep, 0.0)
        h = q * cov * (var_f * inv)
        coef[0, k] = q
        coef[1, k] = h
        coef[2, k] = (q * sf - h * sm) * (1.0 / WINDOW)

    for i in range(5):
        sums[0, i] = jnp.zeros((rows, lanes), jnp.float32)

    @pl.loop(0, HALO + 1)
    def _(p):
        for i, v in enumerate(fields(HALO + p)):
            sums[0, i] += v

    sums[1] = sums[0]
    coefficients(0, HALO)

    def move(way, new, old, k):
        for i, (a, b) in enumerate(zip(fields(new), fields(old))):
            sums[way, i] += a - b
        coefficients(way, k)

    first = planes - 1 - HALO
    for j in range(first):
        move(0, 2 * HALO + 1 + j, HALO + j, HALO + 1 + j)

    acc[...] = jnp.zeros(acc.shape, jnp.float32)
    local[2].wait()

    def output(way, o, new, old):
        total = ksum[way] + coef[:, new] - coef[:, old]
        ksum[way] = total
        left, right = band_dots(total.reshape(3 * rows, lanes), 384, 512, 768)
        boxes[0 : 3 * rows, 0:128] = left
        boxes[0 : 3 * rows, 128:] = right
        boxed = [window_sum(boxes[i * rows : (i + 1) * rows], 0, True) for i in range(3)]
        slope[...] = (-2.0 * SIM_WEIGHT) * (
            plane(0, o + HALO) * boxed[0] - plane(1, o + HALO) * boxed[1] - boxed[2]
        )
        cell = lax.div(o, SPACING)
        weights = spline_weights((o - cell * SPACING).astype(jnp.float32) * (1.0 / SPACING))
        own = slope[pl.ds(y0, height), 0:width]
        for c in range(3):
            v = own * grad[c, o]
            for k in range(4):
                acc[c * cols + cell + k] += weights[k] * v

    meet = HALO - planes // 2
    relay(0)

    @pl.loop(0, HALO)
    def _(s):
        @pl.when(s < HALO - 1)
        def _():
            relay(s + 1)

        ready(0, s)
        move(1, HALO - 1 - s, 2 * HALO - s, HALO - 1 - s)
        ready(1, s)
        move(0, HALO + planes + s, planes - 1 + s, planes + s)

        @pl.when(s == meet)
        def _():
            for way, start in ((1, HALO - meet), (0, planes - HALO - 1 + meet)):
                ksum[way] = coef[:, start]

                @pl.loop(start + 1, start + HALO + 1)
                def _(k):
                    ksum[way] += coef[:, k]

        @pl.when(s >= meet)
        def _():
            low, high = HALO - 1 - s, planes - HALO + s
            output(1, low, low, low + HALO + 1)
            output(0, high, high + HALO, high - 1)

    tables[1].wait()
    tables[2].wait()
    for c in range(3):
        v = acc[c * cols : (c + 1) * cols].reshape(cols * height, width)
        hi, lo = split(v)
        along_x = dot(hi, bx_ref[0]) + dot(hi, bx_ref[1]) + dot(lo, bx_ref[0])
        hi, lo = split(along_x)
        by_hi, by_lo = by_ref[0], by_ref[1]
        along_y = dot(by_hi, hi) + dot(by_lo, hi) + dot(by_hi, lo)
        half = points_y // 2
        for j in range(cols):
            for h in range(2):
                at = j * points_y + h * half
                part[h, j, c] = along_y[at : at + half]

    @pl.when(jnp.logical_not(down))
    def _():
        part[:, 1] += part[:, 0]

    @pl.when(jnp.logical_not(up))
    def _():
        part[:, owned] += part[:, owned + 1] + part[:, owned + 2]

    def p_copy(slot, half, first_row, count, dz, gy):
        return pltpu.make_async_remote_copy(
            part.at[half, pl.ds(first_row, count)],
            arrived.at[slot, pl.ds(0, count)],
            p_send.at[slot], p_recv.at[slot],
            device_id={"gz": z + dz, "gy": gy}, device_id_type=MESH,
        )

    partner = p_copy(0, other, 1, owned, 0, other)
    ups = [p_copy(1, g, 1 + owned, 2, 1, g), p_copy(2, other, 1 + owned, 2, 1, other)]
    downs = [p_copy(3, g, 0, 1, -1, g), p_copy(4, other, 0, 1, -1, other)]

    @pl.when(up)
    def _():
        for copy in ups:
            copy.start()

    @pl.when(down)
    def _():
        for copy in downs:
            copy.start()

    partner.start()
    partner.wait_recv()
    out_ref[...] = part[g, 1 : 1 + owned] + arrived[0]

    @pl.when(down)
    def _():
        for copy in ups:
            copy.wait_recv()
        out_ref[0:2] += arrived[1, 0:2] + arrived[2, 0:2]

    @pl.when(up)
    def _():
        for copy in downs:
            copy.wait_recv()
        out_ref[owned - 1 : owned] += arrived[3, 0:1] + arrived[4, 0:1]

    partner.wait_send()
    y_own.wait_send()

    @pl.when(up)
    def _():
        for copy in ups:
            copy.wait_send()

    @pl.when(down)
    def _():
        for copy in downs:
            copy.wait_send()

    for d in range(2):
        @pl.when(sends[d])
        def _():
            for s in range(HALO):
                z_copy(d, s).wait_send()

        @pl.when(takes[d])
        def _():
            for s in range(HALO):
                y_relay(d, s).wait_send()


def hi_lo(matrix):
    hi = matrix.astype(jnp.bfloat16)
    lo = (matrix - hi.astype(np.float64)).astype(jnp.bfloat16)
    return np.stack([hi, lo])


def band_matrices():
    a, j = np.arange(256)[:, None], np.arange(384)[None, :]
    back = np.concatenate([(j - a)[:, :256], (j - a - 128)[:, 256:]], axis=1)
    ahead = np.concatenate([(a - j)[:, :128], (a + 128 - j)[:, 128:]], axis=1)
    shift = np.concatenate([back, ahead], axis=1)
    return ((shift >= 0) & (shift <= 2 * RADIUS)).astype(jnp.bfloat16)


def local(gz_count, gy_count, fixed_image, moving_image, moving_grad):
    planes, height, width = fixed_image.shape
    points_x, points_y = width // SPACING, gy_count * height // SPACING
    owned = planes // SPACING
    cols = owned + 3
    assert gy_count == 2 and planes >= HALO + 1 and owned >= 2 and height % 8 == 0
    bx = hi_lo(spline_matrix(width, points_x))
    by_all = spline_matrix(gy_count * height, points_y)
    by = np.stack(
        [hi_lo(np.kron(np.eye(cols), by_all[h * height : (h + 1) * height].T)) for h in range(2)]
    )
    rows = height + 2 * HALO
    lanes = (width + HALO + 127) // 128 * 128
    ext_planes = planes + 2 * HALO
    assert lanes == 384 and 256 < width <= 320 and planes % 2 == 0 and planes <= 2 * HALO
    band = band_matrices()
    f32 = jnp.float32
    body = functools.partial(kernel, gz_count, planes, height, width, points_y, points_x)
    vmem, hbm = (pl.BlockSpec(memory_space=m) for m in (pltpu.VMEM, pltpu.HBM))
    half = points_y // 2
    return pl.pallas_call(
        body,
        out_shape=jax.ShapeDtypeStruct((owned, 3, half, points_x), f32),
        in_specs=[hbm] * 6,
        out_specs=vmem,
        scratch_shapes=[
            pltpu.VMEM(bx.shape, jnp.bfloat16),
            pltpu.VMEM(by.shape[1:], jnp.bfloat16),
            pltpu.VMEM(band.shape, jnp.bfloat16),
            pltpu.VMEM((2, planes, height, width), f32),
            pltpu.VMEM((ext_planes, rows, 640), f32),
            pltpu.VMEM(moving_grad.shape, f32),
            pltpu.VMEM((2, 5, rows, lanes), f32),
            pltpu.VMEM((5 * rows, lanes), f32),
            pltpu.VMEM((3, planes + HALO, rows, lanes), f32),
            pltpu.VMEM((2, 3, rows, lanes), f32),
            pltpu.VMEM((rows, lanes), f32),
            pltpu.VMEM((3 * cols, height, width), f32),
            pltpu.VMEM((2, cols, 3, half, points_x), f32),
            pltpu.VMEM((5, owned, 3, half, points_x), f32),
            pltpu.SemaphoreType.DMA((6,)),
            pltpu.SemaphoreType.DMA((2, HALO)),
            pltpu.SemaphoreType.DMA((2, HALO)),
            pltpu.SemaphoreType.DMA((3, HALO)),
            pltpu.SemaphoreType.DMA((3, HALO)),
            pltpu.SemaphoreType.DMA((5,)),
            pltpu.SemaphoreType.DMA((5,)),
        ],
        compiler_params=pltpu.CompilerParams(
            collective_id=0, has_side_effects=True, vmem_limit_bytes=60 * 2**20
        ),
    )(fixed_image, moving_image, moving_grad, jnp.asarray(bx), jnp.asarray(by), jnp.asarray(band))


def solution(mesh):
    in_specs = (P("gz", "gy", None), P("gz", "gy", None), P(None, "gz", "gy", None))
    out_specs = P("gz", None, "gy", None)
    body = functools.partial(local, mesh.shape["gz"], mesh.shape["gy"])
    return jax.shard_map(body, mesh=mesh, in_specs=in_specs, out_specs=out_specs, check_vma=False)
```
